32 devices in a mesh: date: 8 (over z, core), pix: 4 (over y, x).
Axes of the slice: x: 2, y: 2, z: 4, core: 2. Of those that a mesh axis runs over, the one named last changes fastest.
Arguments:
- bin_index: int32 [128, 262144], P('date', 'pix'), may hold values from 0 to 511
- clear_mask: bfloat16 [128, 262144], P('date', 'pix'), may hold values from 0 to 1, as said below
Outputs:
- anomaly: float32 [3, 2048], P(None, 'pix')
- tile_levels: float32 [3], replicated
The draws below stay inside these ranges and needn't reach their ends.
Inputs may be any that keep to these rules, and one draw needn't show every extreme that they name: `clear_mask`: 0 for a cloudy observation, else a positive weight.
All inputs are finite; a program needn't handle non-finite values.
Results may differ from the reference program's by a relative error of at most 0.0003.
Values sent between devices are 32-bit elements; how exact they have to be, the bound alone decides.
No kernel may reach another device: no remote copies, remote signals or barrier semaphores. Data moves between devices by JAX's collectives and lax.ppermute only.
A program may use at most 64 MiB of HBM per device.

```python
import jax
import jax.numpy as jnp
from jax import lax

BINS = 512
BLOCK = 128
DATES = 128
BLOCKS = 2048
PIXELS = 262144


def draw_bin_index(key, part):
    keys = jax.random.split(jax.random.fold_in(key, 11), 8)
    dates = jnp.arange(DATES, dtype=jnp.int32)
    pixels = jnp.arange(PIXELS, dtype=jnp.int32)
    mode_bins = jax.random.randint(keys[0], (BLOCKS, 4), 8, BINS - 8)
    spike_offsets = jax.random.randint(keys[1], (BLOCKS, 4, 4), -7, 8)
    boundaries = jnp.sort(jax.random.randint(keys[2], (BLOCKS, 3), 0, 65), axis=1)
    owner = pixels // BLOCK
    ticket = jax.random.randint(keys[3], (PIXELS,), 0, 64)
    first_mode = jnp.sum((ticket[:, None] >= boundaries[owner]).astype(jnp.int32), axis=1)
    turning = jax.random.randint(keys[4], (PIXELS,), 0, 4)
    season_section = 3 * dates // DATES
    chosen = (first_mode[None] + season_section[:, None] * turning[None]) % 4
    picked = jax.random.randint(keys[5], (DATES, PIXELS), 0, 4)
    mode_slot = owner[None] * 4 + chosen
    located = mode_bins.reshape(-1)[mode_slot] + spike_offsets.reshape(-1)[mode_slot * 4 + picked]
    moded = jnp.clip(located, 0, BINS - 1)
    stray_flag = jax.random.randint(keys[6], (DATES, PIXELS), 0, 3) == 0
    stray_bins = jax.random.randint(keys[7], (DATES, PIXELS), 0, BINS)
    return jnp.where(stray_flag, stray_bins, moded).astype(jnp.int32)


def draw_clear_mask(key, part):
    keys = jax.random.split(jax.random.fold_in(key, 23), 3)
    keeping = jax.random.randint(keys[0], (DATES, BLOCKS, 1), 1, 20)
    rolled = jax.random.randint(keys[1], (DATES, BLOCKS, BLOCK), 0, 20)
    weights = jax.random.uniform(keys[2], (DATES, BLOCKS, BLOCK), jnp.float32, 0.3, 1.0)
    values = jnp.where(rolled < keeping, weights, jnp.zeros((), jnp.float32))
    return values.reshape(DATES, PIXELS).astype(jnp.bfloat16)


def setup_inputs(seed: int = 0) -> dict:
    splits = jax.random.split(jax.random.key(seed), 3)
    return {
        "bin_index": draw_bin_index(jax.random.fold_in(splits[2], 71), 0),
        "clear_mask": draw_clear_mask(jax.random.fold_in(splits[2], 71), 0),
    }


QUANTILES = (0.1, 0.5, 0.9)
LOW_EDGE = -1.0


def percentiles(counts, before, totals):
    target = jnp.stack([quantile * totals + 0.25 for quantile in QUANTILES])
    passed = jnp.clip((target[:, :, None] - before[None]) / jnp.maximum(counts, 1.0)[None], 0.0, 1.0)
    return LOW_EDGE + (2.0 / BINS) * jnp.sum(passed, axis=2)


def reference(bin_index, clear_mask):
    block_base = jnp.arange(PIXELS, dtype=jnp.int32) // BLOCK * BINS

    def add_frame(totals, frame_pair):
        frame_bins, frame_clear = frame_pair
        return totals.at[block_base + frame_bins].add(frame_clear.astype(jnp.float32)), None

    flat_counts, unused = lax.scan(add_frame, jnp.zeros((BLOCKS * BINS,), jnp.float32), (bin_index, clear_mask))
    counts = flat_counts.reshape(BLOCKS, BINS)
    tile_counts = jnp.sum(counts, axis=0)
    tile_before = jnp.cumsum(tile_counts) - tile_counts
    tile_levels = percentiles(tile_counts[None], tile_before[None], jnp.sum(tile_counts)[None])[:, 0]
    block_before = jnp.cumsum(counts, axis=1) - counts
    block_levels = percentiles(counts, block_before, jnp.sum(counts, axis=1))
    return block_levels - tile_levels[:, None], tile_levels
```

```python
import functools

import jax
import jax.numpy as jnp
from jax import lax
from jax.experimental import pallas as pl
from jax.experimental.pallas import tpu as pltpu
from jax.sharding import PartitionSpec as P

BINS = 512
BLOCK = 128
QUANTILES = (0.1, 0.5, 0.9)
LOW_EDGE = -1.0

LANES = 128
LO = 16
HI = BINS // LO
PACK = LANES // HI
TILE_ROWS = LO
INTERLEAVED = 8
FRAME_PAIR = 2


def hist_kernel(where_ref, idx_ref, weight_ref, out_ref, tile_ref, hi_ref, lo_ref, weight32_ref):
    frames, width = idx_ref.shape
    blocks = width // BLOCK
    idx = idx_ref[...]
    hi_ref[...] = (idx // LO).astype(jnp.bfloat16)
    lo_ref[...] = idx % LO
    weight32_ref[...] = weight_ref[...].astype(jnp.float32)
    lo_values = lax.broadcasted_iota(jnp.int32, (LO, BLOCK), 0)
    hi_values = lax.broadcasted_iota(jnp.int32, (HI, BLOCK), 0).astype(jnp.bfloat16)
    one = jnp.ones((HI, BLOCK), jnp.float8_e4m3fn)
    zero = jnp.zeros((HI, BLOCK), jnp.float8_e4m3fn)

    def tables(block, frame):
        lanes = pl.ds(block * BLOCK, BLOCK)
        row = pl.ds(frame, 1)
        lo = jnp.broadcast_to(lo_ref[row, lanes], (LO, BLOCK))
        hi = jnp.broadcast_to(hi_ref[row, lanes], (HI, BLOCK))
        weight = jnp.broadcast_to(weight32_ref[row, lanes], (LO, BLOCK))
        return jnp.where(lo == lo_values, weight, 0.0), jnp.where(hi == hi_values, one, zero)

    tile = jnp.zeros((LO, LANES), jnp.float32)
    for first in range(0, blocks, INTERLEAVED):
        run = range(first, min(first + INTERLEAVED, blocks))
        total = {}
        for frame in range(0, frames, FRAME_PAIR):
            for block in run:
                pairs = [tables(block, f) for f in range(frame, min(frame + FRAME_PAIR, frames))]
                part = lax.dot_general(
                    jnp.concatenate([a for a, _ in pairs], axis=1),
                    jnp.concatenate([b for _, b in pairs], axis=1),
                    (((1,), (1,)), ((), ())),
                    preferred_element_type=jnp.float32,
                )
                total[block] = total[block] + part if frame else part
        for group in range(first // PACK, (run[-1] + 1) // PACK):
            joint = jnp.concatenate([total[group * PACK + j] for j in range(PACK)], axis=1)
            out_ref[0, group] = joint
            tile = tile + joint

    @pl.when(pl.program_id(0) == 0)
    def _():
        tile_ref[...] = tile

    @pl.when(pl.program_id(0) > 0)
    def _():
        tile_ref[...] += tile


def hist(where, bin_index, clear_mask, blocks):
    frames = bin_index.shape[0]
    width = blocks * BLOCK
    runs = where.shape[0]
    groups = blocks // PACK
    taken = pl.BlockSpec((frames, width), lambda i, where: (0, where[i]))
    return pl.pallas_call(
        hist_kernel,
        grid_spec=pltpu.PrefetchScalarGridSpec(
            num_scalar_prefetch=1,
            grid=(runs,),
            in_specs=[taken, taken],
            out_specs=[
                pl.BlockSpec((1, groups, LO, LANES), lambda i, where: (i, 0, 0, 0)),
                pl.BlockSpec((LO, LANES), lambda i, where: (0, 0)),
            ],
            scratch_shapes=[
                pltpu.VMEM((frames, width), jnp.bfloat16),
                pltpu.VMEM((frames, width), jnp.int32),
                pltpu.VMEM((frames, width), jnp.float32),
            ],
        ),
        out_shape=[
            jax.ShapeDtypeStruct((runs, groups, LO, LANES), jnp.float32),
            jax.ShapeDtypeStruct((LO, LANES), jnp.float32),
        ],
        cost_estimate=pl.CostEstimate(
            flops=2 * BINS * frames * width * runs * 8,
            transcendentals=0,
            bytes_accessed=6 * frames * width * runs,
        ),
        name="hist",
    )(where, bin_index, clear_mask)


def split3(x):
    first = x.astype(jnp.bfloat16)
    rest = x - first.astype(jnp.float32)
    second = rest.astype(jnp.bfloat16)
    third = (rest - second.astype(jnp.float32)).astype(jnp.bfloat16)
    return first, second, third


def ones_where(mask):
    return jnp.where(mask, 1.0, 0.0).astype(jnp.bfloat16)


def right(x, ones):
    return sum(jnp.dot(p, ones, preferred_element_type=jnp.float32) for p in split3(x))


def left(ones, x):
    return sum(jnp.dot(ones, p, preferred_element_type=jnp.float32) for p in split3(x))


def iotas(rows, columns):
    shape = (rows, columns)
    return lax.broadcasted_iota(jnp.int32, shape, 0), lax.broadcasted_iota(jnp.int32, shape, 1)


def passed_sums(counts):
    groups = counts.shape[0]
    rows = groups * LO
    r, c = iotas(rows, rows)
    earlier_lo = ones_where((r // LO == c // LO) & (c % LO < r % LO))
    below = left(earlier_lo, counts.reshape(rows, LANES)).reshape(groups, LO, LANES)
    upper = jnp.sum(counts, axis=1)
    r, c = iotas(LANES, LANES)
    same = r // HI == c // HI
    above = right(upper, ones_where(same & (r < c)))
    totals = right(upper, ones_where(same))
    before = below + above[:, None, :]
    width = jnp.maximum(counts, 1.0)
    out = []
    for quantile in QUANTILES:
        target = quantile * totals + 0.25
        out.append(jnp.sum(jnp.clip((target[:, None, :] - before) / width, 0.0, 1.0), axis=1))
    return out


def levels_kernel(place_ref, tile_ref, *refs):
    *part_refs, out_ref = refs
    counts = part_refs[0][...]
    for ref in part_refs[1:]:
        counts = counts + ref[...]
    groups = counts.shape[0]
    blocks = groups * PACK
    sums = jnp.concatenate(passed_sums(counts), axis=0)
    row, offset = place_ref[0], place_ref[1]
    r, c = iotas(LANES, LANES)
    local = c - offset
    spread = right(sums, ones_where((local % PACK == r // HI) & (local >= 0) & (local < blocks)))
    g, c = iotas(groups, LANES)
    local = c - offset
    mine = (local // PACK == g) & (local >= 0) & (local < blocks)
    out_ref[:TILE_ROWS, :] = tile_ref[...]
    out_ref[TILE_ROWS:, :] = jnp.zeros((out_ref.shape[0] - TILE_ROWS, LANES), jnp.float32)
    rows = (out_ref.shape[0] - TILE_ROWS) // len(QUANTILES)
    for n in range(len(QUANTILES)):
        each = jnp.where(mine, spread[n * groups : (n + 1) * groups], 0.0)
        level = LOW_EDGE + 2.0 / BINS * jnp.sum(each, axis=0, keepdims=True)
        k, c = iotas(rows, LANES)
        local = c - offset
        held = (k == row) & (local >= 0) & (local < blocks)
        first = TILE_ROWS + n * rows
        out_ref[first : first + rows, :] = jnp.where(held, jnp.broadcast_to(level, (rows, LANES)), 0.0)


def final_kernel(merged_ref, anomaly_ref, tile_ref):
    r, c = iotas(LANES, LANES)
    tile = right(merged_ref[:TILE_ROWS, :], ones_where(r % HI == c % HI))
    rows = (merged_ref.shape[0] - TILE_ROWS) // len(QUANTILES)
    lane = lax.broadcasted_iota(jnp.int32, (1, LANES), 1)
    for n, sums in enumerate(passed_sums(tile[None])):
        total = jnp.sum(jnp.where(lane < HI, sums, 0.0), axis=1, keepdims=True)
        level = LOW_EDGE + 2.0 / BINS * total
        tile_ref[n : n + 1, :] = jnp.broadcast_to(level, (1, LANES))
        for m in range(rows):
            k = TILE_ROWS + n * rows + m
            anomaly_ref[n : n + 1, m * LANES : (m + 1) * LANES] = merged_ref[k : k + 1, :] - level


def power_of_two(n):
    return n & (n - 1) == 0


def sum_over(x, axis):
    n = lax.axis_size(axis)
    if not power_of_two(n):
        return lax.psum(x, axis)
    step = 1
    while step < n:
        x = x + lax.ppermute(x, axis, [(s, s ^ step) for s in range(n)])
        step *= 2
    return x


def body(bin_index, clear_mask):
    devices = lax.axis_size("date")
    here = lax.axis_index("date")
    blocks_here = bin_index.shape[1] // BLOCK
    owned = blocks_here // devices
    chips = devices // 2
    chip, core = here // 2, here % 2

    def partner(c, k):
        return c ^ k if power_of_two(chips) else (c + k) % chips

    tiles, received = [], []
    kept = None
    for k in reversed(range(chips)):
        base = 2 * partner(chip, k)
        where = jnp.stack([base + 1 - core, base + core]).astype(jnp.int32)
        counts, tile = hist(where, bin_index, clear_mask, owned)
        tiles.append(tile)
        other = lax.ppermute(counts[0], "date", [(s, s ^ 1) for s in range(devices)])
        if k:
            pairs = [(s, 2 * partner(s // 2, k) + s % 2) for s in range(devices)]
            received.append(lax.ppermute(counts[1] + other, "date", pairs))
        else:
            kept = [counts[1], other]
    tile = sum_over(sum(tiles), "pix")

    rows_each = blocks_here // LANES
    rows = -(-(TILE_ROWS + len(QUANTILES) * rows_each) // 8) * 8
    rows = TILE_ROWS + len(QUANTILES) * rows_each
    place = jnp.stack([here * owned // LANES, here * owned % LANES]).astype(jnp.int32)
    vmem = pl.BlockSpec(memory_space=pltpu.VMEM)
    merged = pl.pallas_call(
        levels_kernel,
        in_specs=[pl.BlockSpec(memory_space=pltpu.SMEM)] + [vmem] * (1 + len(kept) + len(received)),
        out_specs=vmem,
        out_shape=jax.ShapeDtypeStruct((rows, LANES), jnp.float32),
        name="levels",
    )(place, tile, *kept, *received)
    merged = sum_over(merged, "date")
    anomaly, tile_levels = pl.pallas_call(
        final_kernel,
        in_specs=[vmem],
        out_specs=[vmem, vmem],
        out_shape=[
            jax.ShapeDtypeStruct((len(QUANTILES), blocks_here), jnp.float32),
            jax.ShapeDtypeStruct((len(QUANTILES), LANES), jnp.float32),
        ],
        name="final",
    )(merged)
    return anomaly, tile_levels[:, 0]


def solution(mesh):
    placed = (P("date", "pix"), P("date", "pix"))
    return jax.shard_map(
        body, mesh=mesh, in_specs=placed, out_specs=(P(None, "pix"), P()), check_vma=False
    )
```

```python
import functools

import jax
import jax.numpy as jnp
from jax import lax
from jax.experimental import pallas as pl
from jax.experimental.pallas import tpu as pltpu
from jax.sharding import PartitionSpec as P

BINS = 512
BLOCK = 128
QUANTILES = (0.1, 0.5, 0.9)
LOW_EDGE = -1.0

LANES = 128
LO_BITS = 4
LO = 1 << LO_BITS
HI = BINS // LO
HI_BITS = HI.bit_length() - 1
PACK = LANES // HI
TILE_ROWS = LO
INTERLEAVED = 8
FRAME_PAIR = 2
PIECE = 32


def power_of_two(n):
    return n & (n - 1) == 0


def partner(chip, k, chips):
    return chip ^ k if power_of_two(chips) else (chip + k) % chips


def hist_kernel(sources, devices, with_tile, here_ref, idx_hbm, weight_hbm, *refs):
    refs = list(refs)
    tile_in = refs.pop(0) if with_tile else None
    outs = [refs.pop(0) for _ in range(2 * len(sources))]
    tile_ref, idx_buf, weight_buf, hi_ref, lo_ref, weight32_ref, sems = refs
    frames = idx_buf.shape[1]
    width = idx_buf.shape[2]
    pieces = idx_buf.shape[0] // len(outs)
    blocks = width // BLOCK
    here = here_ref[0]
    chip, core = here >> 1, here & 1
    copies = []
    for n in range(len(outs)):
        owner = 2 * partner(chip, sources[n // 2], devices // 2) + (core if n % 2 else 1 - core)
        for p in range(pieces):
            at = n * pieces + p
            lanes = pl.ds(pl.multiple_of((owner * pieces + p) * width, width), width)
            pair = (
                pltpu.make_async_copy(idx_hbm.at[:, lanes], idx_buf.at[at], sems.at[0, at]),
                pltpu.make_async_copy(weight_hbm.at[:, lanes], weight_buf.at[at], sems.at[1, at]),
            )
            for copy in pair:
                copy.start()
            copies.append(pair)
    lo_values = lax.broadcasted_iota(jnp.int32, (LO, BLOCK), 0)
    hi_values = lax.broadcasted_iota(jnp.int32, (HI, BLOCK), 0).astype(jnp.bfloat16)
    one = jnp.ones((HI, BLOCK), jnp.float8_e4m3fn)
    zero = jnp.zeros((HI, BLOCK), jnp.float8_e4m3fn)

    def tables(at, block, frame):
        lanes = pl.ds(block * BLOCK, BLOCK)
        row = pl.ds(frame, 1)
        lo = jnp.broadcast_to(lo_ref[at, row, lanes], (LO, BLOCK))
        hi = jnp.broadcast_to(hi_ref[at, row, lanes], (HI, BLOCK))
        weight = jnp.broadcast_to(weight32_ref[at, row, lanes], (LO, BLOCK))
        return jnp.where(lo == lo_values, weight, 0.0), jnp.where(hi == hi_values, one, zero)

    tile = tile_in[...] if with_tile else jnp.zeros((LO, LANES), jnp.float32)
    for at, pair in enumerate(copies):
        for copy in pair:
            copy.wait()
        out_ref = outs[at // pieces]
        for first in range(0, blocks, INTERLEAVED):
            run = range(first, min(first + INTERLEAVED, blocks))
            lanes = pl.ds(first * BLOCK, len(run) * BLOCK)
            idx = idx_buf[at, :, lanes]
            hi_ref[at, :, lanes] = (idx >> LO_BITS).astype(jnp.bfloat16)
            lo_ref[at, :, lanes] = idx & (LO - 1)
            weight32_ref[at, :, lanes] = weight_buf[at, :, lanes].astype(jnp.float32)
            total = {}
            for frame in range(0, frames, FRAME_PAIR):
                for block in run:
                    pairs = [tables(at, block, f) for f in range(frame, min(frame + FRAME_PAIR, frames))]
                    part = lax.dot_general(
                        jnp.concatenate([a for a, _ in pairs], axis=1),
                        jnp.concatenate([b for _, b in pairs], axis=1),
                        (((1,), (1,)), ((), ())),
                        preferred_element_type=jnp.float32,
                    )
                    total[block] = total[block] + part if frame else part
            for group in range(first // PACK, (run[-1] + 1) // PACK):
                joint = jnp.concatenate([total[group * PACK + j] for j in range(PACK)], axis=1)
                out_ref[(at % pieces) * (blocks // PACK) + group] = joint
                tile = tile + joint
    tile_ref[...] = tile


def hist(here, bin_index, clear_mask, sources, devices, tile=None):
    frames, pixels = bin_index.shape
    owned = pixels // BLOCK // devices
    blocks = min(owned, PIECE)
    width = blocks * BLOCK
    slots = 2 * len(sources) * (owned // blocks)
    any_space = pl.BlockSpec(memory_space=pl.ANY)
    vmem = pl.BlockSpec(memory_space=pltpu.VMEM)
    tiles = [] if tile is None else [tile]
    counts = jax.ShapeDtypeStruct((owned // PACK, LO, LANES), jnp.float32)
    return pl.pallas_call(
        functools.partial(hist_kernel, tuple(sources), devices, tile is not None),
        in_specs=[pl.BlockSpec(memory_space=pltpu.SMEM), any_space, any_space] + [vmem] * len(tiles),
        out_specs=[vmem] * (2 * len(sources) + 1),
        out_shape=[counts] * (2 * len(sources)) + [jax.ShapeDtypeStruct((LO, LANES), jnp.float32)],
        scratch_shapes=[
            pltpu.VMEM((slots, frames, width), jnp.int32),
            pltpu.VMEM((slots, frames, width), jnp.bfloat16),
            pltpu.VMEM((slots, frames, width), jnp.bfloat16),
            pltpu.VMEM((slots, frames, width), jnp.int32),
            pltpu.VMEM((slots, frames, width), jnp.float32),
            pltpu.SemaphoreType.DMA((2, slots)),
        ],
        cost_estimate=pl.CostEstimate(
            flops=2 * BINS * frames * width * slots * 8,
            transcendentals=0,
            bytes_accessed=6 * frames * width * slots,
        ),
        name="hist",
    )(here, bin_index, clear_mask, *tiles)


def split3(x):
    first = x.astype(jnp.bfloat16)
    rest = x - first.astype(jnp.float32)
    second = rest.astype(jnp.bfloat16)
    third = (rest - second.astype(jnp.float32)).astype(jnp.bfloat16)
    return first, second, third


def ones_where(mask):
    return jnp.where(mask, 1.0, 0.0).astype(jnp.bfloat16)


def right(x, ones):
    return sum(jnp.dot(p, ones, preferred_element_type=jnp.float32) for p in split3(x))


def left(ones, x):
    return sum(jnp.dot(ones, p, preferred_element_type=jnp.float32) for p in split3(x))


def iotas(rows, columns):
    shape = (rows, columns)
    return lax.broadcasted_iota(jnp.int32, shape, 0), lax.broadcasted_iota(jnp.int32, shape, 1)


def passed_sums(counts):
    groups = counts.shape[0]
    rows = groups * LO
    r, c = iotas(rows, rows)
    earlier_lo = ones_where((r >> LO_BITS == c >> LO_BITS) & (c < r))
    below = left(earlier_lo, counts.reshape(rows, LANES)).reshape(groups, LO, LANES)
    upper = jnp.sum(counts, axis=1)
    r, c = iotas(LANES, LANES)
    same = r >> HI_BITS == c >> HI_BITS
    above = right(upper, ones_where(same & (r < c)))
    totals = right(upper, ones_where(same))
    before = below + above[:, None, :]
    width = jnp.maximum(counts, 1.0)
    out = []
    for quantile in QUANTILES:
        target = quantile * totals + 0.25
        out.append(jnp.sum(jnp.clip((target[:, None, :] - before) / width, 0.0, 1.0), axis=1))
    return out


def levels_kernel(here_ref, tile_ref, tile_other_ref, *refs):
    *part_refs, out_ref = refs
    counts = part_refs[0][...]
    for ref in part_refs[1:]:
        counts = counts + ref[...]
    groups = counts.shape[0]
    blocks = groups * PACK
    sums = jnp.concatenate(passed_sums(counts), axis=0)
    begin = here_ref[0] * blocks
    row, offset = begin // LANES, begin % LANES
    r, c = iotas(LANES, LANES)
    local = c - offset
    spread = right(sums, ones_where((local & (PACK - 1)) == r >> HI_BITS))
    g, c = iotas(groups, LANES)
    local = c - offset
    mine = (local >= g * PACK) & (local < (g + 1) * PACK)
    out_ref[:TILE_ROWS, :] = tile_ref[...] + tile_other_ref[...]
    rows = (out_ref.shape[0] - TILE_ROWS) // len(QUANTILES)
    k, c = iotas(rows, LANES)
    local = c - offset
    held = (k == row) & (local >= 0) & (local < blocks)
    for n in range(len(QUANTILES)):
        each = jnp.where(mine, spread[n * groups : (n + 1) * groups], 0.0)
        level = LOW_EDGE + 2.0 / BINS * jnp.sum(each, axis=0, keepdims=True)
        first = TILE_ROWS + n * rows
        out_ref[first : first + rows, :] = jnp.where(held, jnp.broadcast_to(level, (rows, LANES)), 0.0)


def final_kernel(merged_ref, other_ref, anomaly_ref, tile_ref):
    r, c = iotas(LANES, LANES)
    merged = merged_ref[...] + other_ref[...]
    tile = right(merged[:TILE_ROWS, :], ones_where((r & (HI - 1)) == (c & (HI - 1))))
    rows = (merged.shape[0] - TILE_ROWS) // len(QUANTILES)
    lane = lax.broadcasted_iota(jnp.int32, (1, LANES), 1)
    levels = jnp.zeros((1, LANES), jnp.float32)
    for n, sums in enumerate(passed_sums(tile[None])):
        total = jnp.sum(jnp.where(lane < HI, sums, 0.0), axis=1, keepdims=True)
        level = LOW_EDGE + 2.0 / BINS * total
        levels = jnp.where(lane == n, level, levels)
        for m in range(rows):
            k = TILE_ROWS + n * rows + m
            anomaly_ref[n : n + 1, m * LANES : (m + 1) * LANES] = merged[k : k + 1, :] - level
    tile_ref[...] = levels[0, : len(QUANTILES)]


def swapped(x, axis, step):
    return lax.ppermute(x, axis, [(s, s ^ step) for s in range(lax.axis_size(axis))])


def sum_but_last(x, axis):
    n = lax.axis_size(axis)
    if not power_of_two(n):
        return lax.psum(x, axis), jnp.zeros_like(x)
    step = 1
    while 2 * step < n:
        x = x + swapped(x, axis, step)
        step *= 2
    return x, swapped(x, axis, step) if n > 1 else jnp.zeros_like(x)


def body(bin_index, clear_mask):
    devices = lax.axis_size("date")
    blocks_here = bin_index.shape[1] // BLOCK
    chips = devices // 2
    here = lax.axis_index("date").astype(jnp.int32)[None]

    far = list(reversed(range(2, chips)))
    near = list(reversed(range(min(2, chips))))
    received, mine = [], []
    tile = None
    for sources in (far, near):
        if not sources:
            continue
        *counts, tile = hist(here, bin_index, clear_mask, sources, devices, tile)
        others = [swapped(x, "date", 1) for x in counts[0::2]]
        sums = []
        for k, own, other in zip(sources, counts[1::2], others):
            if k:
                sums.append(own + other)
            else:
                mine = [own, other]
        here, sums = lax.optimization_barrier((here, sums))
        for k, x in zip(sources, sums):
            pairs = [(s, 2 * partner(s // 2, k, chips) + s % 2) for s in range(devices)]
            received.append(lax.ppermute(x, "date", pairs))
    tiles = sum_but_last(tile, "pix")

    rows = TILE_ROWS + len(QUANTILES) * (blocks_here // LANES)
    smem = pl.BlockSpec(memory_space=pltpu.SMEM)
    vmem = pl.BlockSpec(memory_space=pltpu.VMEM)
    parts = mine + received
    merged = pl.pallas_call(
        levels_kernel,
        in_specs=[smem] + [vmem] * (2 + len(parts)),
        out_specs=vmem,
        out_shape=jax.ShapeDtypeStruct((rows, LANES), jnp.float32),
        name="levels",
    )(here, *tiles, *parts)
    return pl.pallas_call(
        final_kernel,
        in_specs=[vmem, vmem],
        out_specs=[vmem, vmem],
        out_shape=[
            jax.ShapeDtypeStruct((len(QUANTILES), blocks_here), jnp.float32),
            jax.ShapeDtypeStruct((len(QUANTILES),), jnp.float32),
        ],
        name="final",
    )(*sum_but_last(merged, "date"))


def solution(mesh):
    placed = (P("date", "pix"), P("date", "pix"))
    return jax.shard_map(
        body, mesh=mesh, in_specs=placed, out_specs=(P(None, "pix"), P()), check_vma=False
    )
```

```python
import functools

import jax
import jax.numpy as jnp
from jax import lax
from jax.experimental import pallas as pl
from jax.experimental.pallas import tpu as pltpu
from jax.sharding import PartitionSpec as P


BINS = 512
BLOCK = 128
QUANTILES = (0.1, 0.5, 0.9)
LOW_EDGE = -1.0

LANES = 128
LO_BITS = 4
LO = 1 << LO_BITS
HI = BINS // LO
HI_BITS = HI.bit_length() - 1
PACK = LANES // HI
TILE_ROWS = LO
INTERLEAVED = 8
FRAME_PAIR = 2
PIECE = 64


def on_chip(shape):
    return pltpu.VMEM(shape, jnp.float32)


def held(x):
    return pltpu.with_memory_space_constraint(x, pltpu.VMEM)


def power_of_two(n):
    return n & (n - 1) == 0


def partner(chip, k, chips):
    return chip ^ k if power_of_two(chips) else (chip + k) % chips


def hist_kernel(counts_here, loads, here_ref, *refs):
    refs = list(refs)
    slots, frames, width = counts_here
    blocks = width // BLOCK
    groups = blocks // PACK
    if loads:
        idx_hbm, weight_hbm = refs[:2]
        out_ref, tile_ref = refs[2:4]
        later = refs[4 : 2 + 2 * len(loads)]
        idx_buf, weight_buf, hi_ref, lo_ref, weight32_ref, sems = refs[2 + 2 * len(loads) :]
        bufs = [(idx_buf, weight_buf)] + [tuple(later[2 * n : 2 * n + 2]) for n in range(len(loads) - 1)]
        here = here_ref[0]
        chip, core = here >> 1, here & 1

        def copies(call, at, lanes):
            return (
                pltpu.make_async_copy(idx_hbm.at[:, lanes], bufs[call][0].at[at], sems.at[0, call, at]),
                pltpu.make_async_copy(weight_hbm.at[:, lanes], bufs[call][1].at[at], sems.at[1, call, at]),
            )

        def started(call):
            sources, keep, pieces, chips = loads[call]
            for n, k in enumerate(sources):
                owner = 2 * partner(chip, k, chips) + (core if keep else 1 - core)
                for p in range(pieces):
                    start = pl.multiple_of((owner * pieces + p) * width, width)
                    for copy in copies(call, n * pieces + p, pl.ds(start, width)):
                        copy.start()

        started(0)
        tile_ref[...] = jnp.zeros((LO, LANES), jnp.float32)
    else:
        idx_buf, weight_buf, tile_in, out_ref, tile_ref, hi_ref, lo_ref, weight32_ref = refs
        tile_ref[...] = tile_in[...]
    lo_values = lax.broadcasted_iota(jnp.int32, (LO, BLOCK), 0)
    hi_values = lax.broadcasted_iota(jnp.int32, (HI, BLOCK), 0).astype(jnp.bfloat16)
    one = jnp.ones((HI, BLOCK), jnp.float8_e4m3fn)
    zero = jnp.zeros((HI, BLOCK), jnp.float8_e4m3fn)

    def tables(block, frame):
        lanes = pl.ds(block * BLOCK, BLOCK)
        row = pl.ds(frame, 1)
        lo = jnp.broadcast_to(lo_ref[row, lanes], (LO, BLOCK))
        hi = jnp.broadcast_to(hi_ref[row, lanes], (HI, BLOCK))
        weight = jnp.broadcast_to(weight32_ref[row, lanes], (LO, BLOCK))
        return jnp.where(lo == lo_values, weight, 0.0), jnp.where(hi == hi_values, one, zero)

    def piece(at, unused):
        if loads:
            for copy in copies(0, at, pl.ds(0, width)):
                copy.wait()

            @pl.when(at == 0)
            def _():
                for call in range(1, len(loads)):
                    started(call)

        idx = idx_buf[at]
        hi_ref[...] = (idx >> LO_BITS).astype(jnp.bfloat16)
        lo_ref[...] = idx & (LO - 1)
        weight32_ref[...] = weight_buf[at].astype(jnp.float32)
        tile = tile_ref[...]
        for first in range(0, blocks, INTERLEAVED):
            run = range(first, min(first + INTERLEAVED, blocks))
            total = {}
            for frame in range(0, frames, FRAME_PAIR):
                for block in run:
                    pairs = [tables(block, f) for f in range(frame, min(frame + FRAME_PAIR, frames))]
                    part = lax.dot_general(
                        jnp.concatenate([a for a, _ in pairs], axis=1),
                        jnp.concatenate([b for _, b in pairs], axis=1),
                        (((1,), (1,)), ((), ())),
                        preferred_element_type=jnp.float32,
                    )
                    total[block] = total[block] + part if frame else part
            for group in range(len(run) // PACK):
                each = [total[run[group * PACK + j]] for j in range(PACK)]
                joint = jnp.concatenate(each, axis=1)
                out_ref[at * groups + first // PACK + group] = joint
                tile = tile + joint
        tile_ref[...] = tile
        return unused

    lax.fori_loop(0, slots, piece, 0)
    for call in range(1, len(loads)):
        sources, _, pieces, _ = loads[call]
        for at in range(len(sources) * pieces):
            for copy in copies(call, at, pl.ds(0, width)):
                copy.wait()


def hist(here, frames, slots, width, operands, loads=()):
    in_hbm = pl.BlockSpec(memory_space=pltpu.HBM)
    vmem = pl.BlockSpec(memory_space=pltpu.VMEM)
    groups = slots * (width // BLOCK) // PACK
    outs = [on_chip((groups, LO, LANES)), on_chip((LO, LANES))]
    scratch = [
        pltpu.VMEM((frames, width), jnp.bfloat16),
        pltpu.VMEM((frames, width), jnp.int32),
        pltpu.VMEM((frames, width), jnp.float32),
    ]
    if loads:
        for sources, _, pieces, _ in loads[1:]:
            shape = (len(sources) * pieces, frames, width)
            outs += [pltpu.VMEM(shape, jnp.int32), pltpu.VMEM(shape, jnp.bfloat16)]
        most = max(len(sources) * pieces for sources, _, pieces, _ in loads)
        scratch = [
            pltpu.VMEM((slots, frames, width), jnp.int32),
            pltpu.VMEM((slots, frames, width), jnp.bfloat16),
            *scratch,
            pltpu.SemaphoreType.DMA((2, len(loads), most)),
        ]
    return pl.pallas_call(
        functools.partial(hist_kernel, (slots, frames, width), tuple(loads)),
        in_specs=[pl.BlockSpec(memory_space=pltpu.SMEM)]
        + [in_hbm if loads else vmem] * len(operands),
        out_specs=[vmem] * len(outs),
        out_shape=outs,
        scratch_shapes=scratch,
        compiler_params=pltpu.CompilerParams(vmem_limit_bytes=24 << 20),
        cost_estimate=pl.CostEstimate(
            flops=2 * BINS * frames * width * slots * 8,
            transcendentals=0,
            bytes_accessed=6 * frames * width * slots,
        ),
        name="hist",
    )(here, *operands)


def split3(x):
    first = x.astype(jnp.bfloat16)
    rest = x - first.astype(jnp.float32)
    second = rest.astype(jnp.bfloat16)
    third = (rest - second.astype(jnp.float32)).astype(jnp.bfloat16)
    return first, second, third


def ones_where(mask):
    return jnp.where(mask, 1.0, 0.0).astype(jnp.bfloat16)


def right(x, ones):
    return sum(jnp.dot(p, ones, preferred_element_type=jnp.float32) for p in split3(x))


def left(ones, x):
    return sum(jnp.dot(ones, p, preferred_element_type=jnp.float32) for p in split3(x))


def iotas(rows, columns):
    shape = (rows, columns)
    return lax.broadcasted_iota(jnp.int32, shape, 0), lax.broadcasted_iota(jnp.int32, shape, 1)


def passed_sums(counts):
    groups = counts.shape[0]
    rows = groups * LO
    r, c = iotas(rows, rows)
    earlier_lo = ones_where((r >> LO_BITS == c >> LO_BITS) & (c < r))
    below = left(earlier_lo, counts.reshape(rows, LANES)).reshape(groups, LO, LANES)
    upper = jnp.sum(counts, axis=1)
    r, c = iotas(LANES, LANES)
    same = r >> HI_BITS == c >> HI_BITS
    above = right(upper, ones_where(same & (r < c)))
    totals = right(upper, ones_where(same))
    before = below + above[:, None, :]
    inverse = 1.0 / jnp.maximum(counts, 1.0)
    out = []
    for quantile in QUANTILES:
        target = quantile * totals + 0.25
        out.append(jnp.sum(jnp.clip((target[:, None, :] - before) * inverse, 0.0, 1.0), axis=1))
    return out


def levels_kernel(here_ref, tile_ref, tile_other_ref, *refs):
    *part_refs, out_ref = refs
    size = part_refs[-1].shape[0]
    counts = None
    for ref in part_refs:
        part = ref[ref.shape[0] - size :]
        counts = part if counts is None else counts + part
    groups = counts.shape[0]
    blocks = groups * PACK
    sums = jnp.concatenate(passed_sums(counts), axis=0)
    begin = here_ref[0] * blocks
    row, offset = begin // LANES, begin % LANES
    r, c = iotas(LANES, LANES)
    local = c - offset
    spread = right(sums, ones_where((local & (PACK - 1)) == r >> HI_BITS))
    g, c = iotas(groups, LANES)
    local = c - offset
    mine = (local >= g * PACK) & (local < (g + 1) * PACK)
    out_ref[:TILE_ROWS, :] = tile_ref[...] + tile_other_ref[...]
    rows = (out_ref.shape[0] - TILE_ROWS) // len(QUANTILES)
    k, c = iotas(rows, LANES)
    local = c - offset
    held = (k == row) & (local >= 0) & (local < blocks)
    for n in range(len(QUANTILES)):
        each = jnp.where(mine, spread[n * groups : (n + 1) * groups], 0.0)
        level = LOW_EDGE + 2.0 / BINS * jnp.sum(each, axis=0, keepdims=True)
        first = TILE_ROWS + n * rows
        out_ref[first : first + rows, :] = jnp.where(held, jnp.broadcast_to(level, (rows, LANES)), 0.0)


def final_kernel(merged_ref, other_ref, anomaly_ref, tile_ref):
    r, c = iotas(LANES, LANES)
    merged = merged_ref[...] + other_ref[...]
    tile = right(merged[:TILE_ROWS, :], ones_where((r & (HI - 1)) == (c & (HI - 1))))
    rows = (merged.shape[0] - TILE_ROWS) // len(QUANTILES)
    lane = lax.broadcasted_iota(jnp.int32, (1, LANES), 1)
    levels = jnp.zeros((1, LANES), jnp.float32)
    for n, sums in enumerate(passed_sums(tile[None])):
        total = jnp.sum(jnp.where(lane < HI, sums, 0.0), axis=1, keepdims=True)
        level = LOW_EDGE + 2.0 / BINS * total
        levels = jnp.where(lane == n, level, levels)
        for m in range(rows):
            k = TILE_ROWS + n * rows + m
            anomaly_ref[n : n + 1, m * LANES : (m + 1) * LANES] = merged[k : k + 1, :] - level
    tile_ref[...] = levels[0, : len(QUANTILES)]


def swapped(x, axis, step):
    return lax.ppermute(x, axis, [(s, s ^ step) for s in range(lax.axis_size(axis))])


def sum_but_last(x, axis):
    n = lax.axis_size(axis)
    if not power_of_two(n):
        return lax.psum(x, axis), jnp.zeros_like(x)
    step = 1
    while 2 * step < n:
        other = swapped(x, axis, step)
        x = x + other
        step *= 2
    return x, swapped(x, axis, step) if n > 1 else jnp.zeros_like(x)


def body(bin_index, clear_mask):
    devices = lax.axis_size("date")
    blocks_here = bin_index.shape[1] // BLOCK
    chips = devices // 2
    here = lax.axis_index("date").astype(jnp.int32)[None]

    frames = bin_index.shape[0]
    owned = blocks_here // devices
    owned_groups = owned // PACK
    blocks = min(owned, PIECE)
    width = blocks * BLOCK
    pieces = owned // blocks
    far = tuple(reversed(range(2, chips)))
    near = tuple(reversed(range(min(2, chips))))
    loads = [(k, keep, pieces, chips) for k in (far, near) if k for keep in (False, True)]
    stages = [k for k in (far, near) if k]

    args = [pltpu.with_memory_space_constraint(x, pltpu.HBM) for x in (bin_index, clear_mask)]
    received, mine = [], []
    tile, later = None, None
    for sources in stages:
        counts = []
        for keep in range(2):
            slots = len(sources) * pieces
            if later is None:
                part, tile, *later = hist(here, frames, slots, width, args, loads)
            else:
                operands = [held(x) for x in (*later[:2], tile)]
                later = later[2:]
                part, tile = hist(here, frames, slots, width, operands)
            counts.append(part)
            if not keep:
                other = swapped(part, "date", 1)
        own = counts[1]
        for n, k in enumerate(sources):
            rows = slice(n * owned_groups, (n + 1) * owned_groups)
            if k:
                total = own[rows] + other[rows]
                pairs = [(s, 2 * partner(s // 2, k, chips) + s % 2) for s in range(devices)]
                received.append(lax.ppermute(total, "date", pairs))
            else:
                mine = [own, other]
    tiles = sum_but_last(tile, "pix")

    rows = TILE_ROWS + len(QUANTILES) * (blocks_here // LANES)
    smem = pl.BlockSpec(memory_space=pltpu.SMEM)
    vmem = pl.BlockSpec(memory_space=pltpu.VMEM)
    parts = mine + received
    merged = pl.pallas_call(
        levels_kernel,
        in_specs=[smem] + [vmem] * (2 + len(parts)),
        out_specs=vmem,
        out_shape=on_chip((rows, LANES)),
        name="levels",
    )(here, *[held(x) for x in (*tiles, *parts)])
    return pl.pallas_call(
        final_kernel,
        in_specs=[vmem, vmem],
        out_specs=[vmem, vmem],
        out_shape=[
            jax.ShapeDtypeStruct((len(QUANTILES), blocks_here), jnp.float32),
            jax.ShapeDtypeStruct((len(QUANTILES),), jnp.float32),
        ],
        name="final",
    )(*[held(x) for x in sum_but_last(merged, "date")])


def solution(mesh):
    placed = (P("date", "pix"), P("date", "pix"))
    return jax.shard_map(body, mesh=mesh, in_specs=placed, out_specs=(P(None, "pix"), P()), check_vma=False)
```

```python
import functools

import jax
import jax.numpy as jnp
from jax import lax
from jax.experimental import pallas as pl
from jax.experimental.pallas import tpu as pltpu
from jax.sharding import PartitionSpec as P


BINS = 512
BLOCK = 128
QUANTILES = (0.1, 0.5, 0.9)
LOW_EDGE = -1.0

LANES = 128
LO_BITS = 4
LO = 1 << LO_BITS
HI = BINS // LO
HI_BITS = HI.bit_length() - 1
PACK = LANES // HI
TILE_ROWS = LO
INTERLEAVED = 8
FRAME_PAIR = 2
PIECE = 64


def on_chip(shape):
    return pltpu.VMEM(shape, jnp.float32)


def held(x):
    return pltpu.with_memory_space_constraint(x, pltpu.VMEM)


def power_of_two(n):
    return n & (n - 1) == 0


def partner(chip, k, chips):
    return chip ^ k if power_of_two(chips) else (chip + k) % chips


def hist_kernel(counts_here, own, loads, here_ref, *refs):
    refs = list(refs)
    slots, frames, width = counts_here
    blocks = width // BLOCK
    groups = blocks // PACK
    idx_hbm, weight_hbm = (refs.pop(0), refs.pop(0)) if own or loads else (None, None)
    idx_buf, weight_buf, tile_in = (None,) * 3 if own else (refs.pop(0), refs.pop(0), refs.pop(0))
    out_ref, tile_ref = refs.pop(0), refs.pop(0)
    bufs = [(refs.pop(0), refs.pop(0)) for _ in loads]
    if own:
        idx_buf, weight_buf = refs.pop(0), refs.pop(0)
    hi_ref, lo_ref, weight32_ref = refs[:3]
    bufs.append((idx_buf, weight_buf))
    wanted = [*loads, own]
    if own or loads:
        sems = refs[3]
        here = here_ref[0]
        chip, core = here >> 1, here & 1

        def copies(call, at, lanes):
            return (
                pltpu.make_async_copy(idx_hbm.at[:, lanes], bufs[call][0].at[at], sems.at[0, call, at]),
                pltpu.make_async_copy(weight_hbm.at[:, lanes], bufs[call][1].at[at], sems.at[1, call, at]),
            )

        def started(call):
            sources, keep, pieces, chips = wanted[call]
            for n, k in enumerate(sources):
                owner = 2 * partner(chip, k, chips) + (core if keep else 1 - core)
                for p in range(pieces):
                    start = pl.multiple_of((owner * pieces + p) * width, width)
                    for copy in copies(call, n * pieces + p, pl.ds(start, width)):
                        copy.start()

        if own:
            started(len(loads))
        else:
            for call in range(len(loads)):
                started(call)
    tile_ref[...] = jnp.zeros((LO, LANES), jnp.float32) if own else tile_in[...]
    lo_values = lax.broadcasted_iota(jnp.int32, (LO, BLOCK), 0)
    hi_values = lax.broadcasted_iota(jnp.int32, (HI, BLOCK), 0).astype(jnp.bfloat16)
    one = jnp.ones((HI, BLOCK), jnp.float8_e4m3fn)
    zero = jnp.zeros((HI, BLOCK), jnp.float8_e4m3fn)

    def tables(block, frame):
        lanes = pl.ds(block * BLOCK, BLOCK)
        row = pl.ds(frame, 1)
        lo = jnp.broadcast_to(lo_ref[row, lanes], (LO, BLOCK))
        hi = jnp.broadcast_to(hi_ref[row, lanes], (HI, BLOCK))
        weight = jnp.broadcast_to(weight32_ref[row, lanes], (LO, BLOCK))
        return jnp.where(lo == lo_values, weight, 0.0), jnp.where(hi == hi_values, one, zero)

    def piece(at, unused):
        if own:
            for copy in copies(len(loads), at, pl.ds(0, width)):
                copy.wait()

            @pl.when(at == 0)
            def _():
                for call in range(len(loads)):
                    started(call)

        idx = idx_buf[at]
        hi_ref[...] = (idx >> LO_BITS).astype(jnp.bfloat16)
        lo_ref[...] = idx & (LO - 1)
        weight32_ref[...] = weight_buf[at].astype(jnp.float32)
        tile = tile_ref[...]
        for first in range(0, blocks, INTERLEAVED):
            run = range(first, min(first + INTERLEAVED, blocks))
            total = {}
            for frame in range(0, frames, FRAME_PAIR):
                for block in run:
                    pairs = [tables(block, f) for f in range(frame, min(frame + FRAME_PAIR, frames))]
                    part = lax.dot_general(
                        jnp.concatenate([a for a, _ in pairs], axis=1),
                        jnp.concatenate([b for _, b in pairs], axis=1),
                        (((1,), (1,)), ((), ())),
                        preferred_element_type=jnp.float32,
                    )
                    total[block] = total[block] + part if frame else part
            for group in range(len(run) // PACK):
                each = [total[run[group * PACK + j]] for j in range(PACK)]
                joint = jnp.concatenate(each, axis=1)
                out_ref[at * groups + first // PACK + group] = joint
                tile = tile + joint
        tile_ref[...] = tile
        return unused

    lax.fori_loop(0, slots, piece, 0)
    for call in range(len(loads)):
        sources, _, pieces, _ = loads[call]
        for at in range(len(sources) * pieces):
            for copy in copies(call, at, pl.ds(0, width)):
                copy.wait()


def hist(here, frames, slots, width, in_place, operands, own, loads):
    in_hbm = pl.BlockSpec(memory_space=pltpu.HBM)
    vmem = pl.BlockSpec(memory_space=pltpu.VMEM)
    groups = slots * (width // BLOCK) // PACK
    outs = [on_chip((groups, LO, LANES)), on_chip((LO, LANES))]
    scratch = [
        pltpu.VMEM((frames, width), jnp.bfloat16),
        pltpu.VMEM((frames, width), jnp.int32),
        pltpu.VMEM((frames, width), jnp.float32),
    ]
    wanted = [*loads, own] if own else list(loads)
    for sources, _, pieces, _ in loads:
        shape = (len(sources) * pieces, frames, width)
        outs += [pltpu.VMEM(shape, jnp.int32), pltpu.VMEM(shape, jnp.bfloat16)]
    if own:
        scratch = [
            pltpu.VMEM((slots, frames, width), jnp.int32),
            pltpu.VMEM((slots, frames, width), jnp.bfloat16),
            *scratch,
        ]
    if wanted:
        most = max(len(sources) * pieces for sources, _, pieces, _ in wanted)
        scratch.append(pltpu.SemaphoreType.DMA((2, len(wanted), most)))
    else:
        in_place = ()
    return pl.pallas_call(
        functools.partial(hist_kernel, (slots, frames, width), own, tuple(loads)),
        in_specs=[pl.BlockSpec(memory_space=pltpu.SMEM)]
        + [in_hbm] * len(in_place)
        + [vmem] * len(operands),
        out_specs=[vmem] * len(outs),
        out_shape=outs,
        scratch_shapes=scratch,
        compiler_params=pltpu.CompilerParams(vmem_limit_bytes=24 << 20),
        cost_estimate=pl.CostEstimate(
            flops=2 * BINS * frames * width * slots * 8,
            transcendentals=0,
            bytes_accessed=6 * frames * width * slots,
        ),
        name="hist",
    )(here, *in_place, *operands)


def split3(x):
    first = x.astype(jnp.bfloat16)
    rest = x - first.astype(jnp.float32)
    second = rest.astype(jnp.bfloat16)
    third = (rest - second.astype(jnp.float32)).astype(jnp.bfloat16)
    return first, second, third


def ones_where(mask):
    return jnp.where(mask, 1.0, 0.0).astype(jnp.bfloat16)


def right(x, ones):
    return sum(jnp.dot(p, ones, preferred_element_type=jnp.float32) for p in split3(x))


def left(ones, x):
    return sum(jnp.dot(ones, p, preferred_element_type=jnp.float32) for p in split3(x))


def iotas(rows, columns):
    shape = (rows, columns)
    return lax.broadcasted_iota(jnp.int32, shape, 0), lax.broadcasted_iota(jnp.int32, shape, 1)


def passed_sums(counts):
    groups = counts.shape[0]
    rows = groups * LO
    r, c = iotas(rows, rows)
    earlier_lo = ones_where((r >> LO_BITS == c >> LO_BITS) & (c < r))
    below = left(earlier_lo, counts.reshape(rows, LANES)).reshape(groups, LO, LANES)
    upper = jnp.sum(counts, axis=1)
    r, c = iotas(LANES, LANES)
    same = r >> HI_BITS == c >> HI_BITS
    above = right(upper, ones_where(same & (r < c)))
    totals = right(upper, ones_where(same))
    before = below + above[:, None, :]
    inverse = 1.0 / jnp.maximum(counts, 1.0)
    out = []
    for quantile in QUANTILES:
        target = quantile * totals + 0.25
        out.append(jnp.sum(jnp.clip((target[:, None, :] - before) * inverse, 0.0, 1.0), axis=1))
    return out


def levels_kernel(here_ref, tile_ref, tile_other_ref, *refs):
    *part_refs, out_ref = refs
    size = part_refs[-1].shape[0]
    counts = None
    for ref in part_refs:
        part = ref[ref.shape[0] - size :]
        counts = part if counts is None else counts + part
    groups = counts.shape[0]
    blocks = groups * PACK
    sums = jnp.concatenate(passed_sums(counts), axis=0)
    begin = here_ref[0] * blocks
    row, offset = begin // LANES, begin % LANES
    r, c = iotas(LANES, LANES)
    local = c - offset
    spread = right(sums, ones_where((local & (PACK - 1)) == r >> HI_BITS))
    g, c = iotas(groups, LANES)
    local = c - offset
    mine = (local >= g * PACK) & (local < (g + 1) * PACK)
    out_ref[:TILE_ROWS, :] = tile_ref[...] + tile_other_ref[...]
    rows = (out_ref.shape[0] - TILE_ROWS) // len(QUANTILES)
    k, c = iotas(rows, LANES)
    local = c - offset
    held = (k == row) & (local >= 0) & (local < blocks)
    for n in range(len(QUANTILES)):
        each = jnp.where(mine, spread[n * groups : (n + 1) * groups], 0.0)
        level = LOW_EDGE + 2.0 / BINS * jnp.sum(each, axis=0, keepdims=True)
        first = TILE_ROWS + n * rows
        out_ref[first : first + rows, :] = jnp.where(held, jnp.broadcast_to(level, (rows, LANES)), 0.0)


def final_kernel(merged_ref, other_ref, anomaly_ref, tile_ref):
    r, c = iotas(LANES, LANES)
    merged = merged_ref[...] + other_ref[...]
    tile = right(merged[:TILE_ROWS, :], ones_where((r & (HI - 1)) == (c & (HI - 1))))
    rows = (merged.shape[0] - TILE_ROWS) // len(QUANTILES)
    lane = lax.broadcasted_iota(jnp.int32, (1, LANES), 1)
    levels = jnp.zeros((1, LANES), jnp.float32)
    for n, sums in enumerate(passed_sums(tile[None])):
        total = jnp.sum(jnp.where(lane < HI, sums, 0.0), axis=1, keepdims=True)
        level = LOW_EDGE + 2.0 / BINS * total
        levels = jnp.where(lane == n, level, levels)
        for m in range(rows):
            k = TILE_ROWS + n * rows + m
            anomaly_ref[n : n + 1, m * LANES : (m + 1) * LANES] = merged[k : k + 1, :] - level
    tile_ref[...] = levels[0, : len(QUANTILES)]


def swapped(x, axis, step):
    return lax.ppermute(x, axis, [(s, s ^ step) for s in range(lax.axis_size(axis))])


def sum_but_last(x, axis):
    n = lax.axis_size(axis)
    if not power_of_two(n):
        return lax.psum(x, axis), jnp.zeros_like(x)
    step = 1
    while 2 * step < n:
        other = swapped(x, axis, step)
        x = x + other
        step *= 2
    return x, swapped(x, axis, step) if n > 1 else jnp.zeros_like(x)


def body(bin_index, clear_mask):
    devices = lax.axis_size("date")
    blocks_here = bin_index.shape[1] // BLOCK
    chips = devices // 2
    here = lax.axis_index("date").astype(jnp.int32)[None]

    frames = bin_index.shape[0]
    owned = blocks_here // devices
    owned_groups = owned // PACK
    blocks = min(owned, PIECE)
    width = blocks * BLOCK
    pieces = owned // blocks
    far = tuple(reversed(range(2, chips)))
    near = tuple(reversed(range(min(2, chips))))
    loads = [(k, keep, pieces, chips) for k in (far, near) if k for keep in (False, True)]
    stages = [k for k in (far, near) if k]

    args = [pltpu.with_memory_space_constraint(x, pltpu.HBM) for x in (bin_index, clear_mask)]
    received, mine = [], []
    tile, later = None, None
    for stage, sources in enumerate(stages):
        counts = []
        for keep in range(2):
            slots = len(sources) * pieces
            calls = loads[2 * stage + keep :]
            own = calls[0] if later is None else None
            coming = {0: calls[1:2], 1: calls[1:]}.get(2 * stage + keep, [])
            operands = [] if own else [held(x) for x in (*later[:2], tile)]
            part, tile, *brought = hist(here, frames, slots, width, args, operands, own, coming)
            later = (later or [])[2:] + brought
            counts.append(part)
            if not keep:
                other = swapped(part, "date", 1)
        own = counts[1]
        for n, k in enumerate(sources):
            rows = slice(n * owned_groups, (n + 1) * owned_groups)
            if k:
                total = own[rows] + other[rows]
                pairs = [(s, 2 * partner(s // 2, k, chips) + s % 2) for s in range(devices)]
                received.append(lax.ppermute(total, "date", pairs))
            else:
                mine = [own, other]
    tiles = sum_but_last(tile, "pix")

    rows = TILE_ROWS + len(QUANTILES) * (blocks_here // LANES)
    smem = pl.BlockSpec(memory_space=pltpu.SMEM)
    vmem = pl.BlockSpec(memory_space=pltpu.VMEM)
    parts = mine + received
    merged = pl.pallas_call(
        levels_kernel,
        in_specs=[smem] + [vmem] * (2 + len(parts)),
        out_specs=vmem,
        out_shape=on_chip((rows, LANES)),
        name="levels",
    )(here, *[held(x) for x in (*tiles, *parts)])
    return pl.pallas_call(
        final_kernel,
        in_specs=[vmem, vmem],
        out_specs=[vmem, vmem],
        out_shape=[
            jax.ShapeDtypeStruct((len(QUANTILES), blocks_here), jnp.float32),
            jax.ShapeDtypeStruct((len(QUANTILES),), jnp.float32),
        ],
        name="final",
    )(*[held(x) for x in sum_but_last(merged, "date")])


def solution(mesh):
    placed = (P("date", "pix"), P("date", "pix"))
    return jax.shard_map(body, mesh=mesh, in_specs=placed, out_specs=(P(None, "pix"), P()), check_vma=False)
```
